8 devices in a mesh: dp: 2 (over z, y), tp: 4 (over x, core).
Axes of the slice: x: 2, y: 2, z: 1, core: 2. Of those that a mesh axis runs over, the one named last changes fastest.
Arguments:
- x_tokens: bfloat16 [16, 512, 4096], P('dp', 'tp'), parts along dimension 0
- ln1_gain: float32 [2, 4096], replicated
- ln1_bias: float32 [2, 4096], replicated
- ln2_gain: float32 [2, 4096], replicated
- ln2_bias: float32 [2, 4096], replicated
- w_qkv: bfloat16 [2, 4096, 3, 32, 128], P(None, None, None, 'tp')
- w_out: bfloat16 [2, 32, 128, 4096], P(None, 'tp')
- b_out: float32 [2, 4096], replicated
- w_up: bfloat16 [2, 4096, 16384], P(None, None, 'tp')
- b_up: float32 [2, 16384], P(None, 'tp')
- w_down: bfloat16 [2, 16384, 4096], P(None, 'tp')
- b_down: float32 [2, 4096], replicated
Outputs:
- output: bfloat16 [16, 512, 4096], P('dp', 'tp'), parts along dimension 0
There are 2 independent parts. The reference program is written for one: setup_inputs(seed, part) draws one part's arguments, and reference() takes and returns one part's arrays. A program takes and returns all parts, laid end to end along the dimension named above; an argument that names none is the same for every part.
All inputs are finite; a program needn't handle non-finite values.
Results may differ from the reference program's by a relative error of at most 0.010747.
Values are sent between devices in bfloat16 or wider.
A program may use at most 1 GiB of HBM per device.

```python
import math
import jax
import jax.numpy as jnp
from jax import lax

BATCH = 8
SEQ_LEN = 512
D_MODEL = 4096
HEADS = 32
HEAD_DIM = 128
D_FF = 16384
LAYERS = 2


def setup_inputs(seed: int = 0, part: int = 0) -> dict:
    base_key = jax.random.key(seed)
    part_key = jax.random.fold_in(base_key, part)
    row_key, tok_key = jax.random.split(part_key)
    keys = jax.random.split(base_key, 11)
    row_scale = 0.5 + jax.random.uniform(row_key, (BATCH, SEQ_LEN, 1), jnp.float32)
    tokens = jax.random.normal(tok_key, (BATCH, SEQ_LEN, D_MODEL), jnp.float32) * row_scale
    qk_gain = (math.log(SEQ_LEN) / 2.0) ** 0.25
    attn_level = math.sqrt((1.0 + 0.5 * math.log(SEQ_LEN)) / math.sqrt(SEQ_LEN))
    out_gain = 0.5 / attn_level
    proj_gain = jnp.array([qk_gain, qk_gain, 1.0], jnp.float32).reshape(1, 1, 3, 1, 1)
    vec_shape = (LAYERS, D_MODEL)
    w_qkv = jax.random.normal(keys[4], (LAYERS, D_MODEL, 3, HEADS, HEAD_DIM), jnp.float32) * proj_gain * D_MODEL ** -0.5
    w_out = jax.random.normal(keys[5], (LAYERS, HEADS, HEAD_DIM, D_MODEL), jnp.float32) * (out_gain * D_MODEL ** -0.5)
    w_up = jax.random.normal(keys[7], (LAYERS, D_MODEL, D_FF), jnp.float32) * D_MODEL ** -0.5
    w_down = jax.random.normal(keys[9], (LAYERS, D_FF, D_MODEL), jnp.float32) * (0.8 * D_FF ** -0.5)
    return {
        "x_tokens": tokens.astype(jnp.bfloat16),
        "ln1_gain": 1.0 + 0.2 * jax.random.normal(keys[0], vec_shape, jnp.float32),
        "ln1_bias": 0.2 * jax.random.normal(keys[1], vec_shape, jnp.float32),
        "ln2_gain": 1.0 + 0.2 * jax.random.normal(keys[2], vec_shape, jnp.float32),
        "ln2_bias": 0.2 * jax.random.normal(keys[3], vec_shape, jnp.float32),
        "w_qkv": w_qkv.astype(jnp.bfloat16),
        "w_out": w_out.astype(jnp.bfloat16),
        "b_out": 0.2 * jax.random.normal(keys[6], vec_shape, jnp.float32),
        "w_up": w_up.astype(jnp.bfloat16),
        "b_up": 0.3 * jax.random.normal(keys[8], (LAYERS, D_FF), jnp.float32),
        "w_down": w_down.astype(jnp.bfloat16),
        "b_down": 0.2 * jax.random.normal(keys[10], vec_shape, jnp.float32),
    }


def layer_norm(resid, gain, shift):
    row_mean = jnp.mean(resid, axis=-1, keepdims=True)
    centered = resid - row_mean
    variance = jnp.mean(centered * centered, axis=-1, keepdims=True)
    return (centered * lax.rsqrt(variance + 1e-5) * gain + shift).astype(jnp.bfloat16)


def attention_head(head_parts):
    queries, keys_all, values_all = head_parts
    scores = jnp.einsum("bqe,bke->bqk", queries.astype(jnp.float32), keys_all.astype(jnp.float32)) / math.sqrt(HEAD_DIM)
    positions = jnp.arange(SEQ_LEN)
    causal = positions[:, None] >= positions[None, :]
    scores = jnp.where(causal, scores, -1e30)
    attn_probs = jax.nn.softmax(scores, axis=-1).astype(jnp.bfloat16)
    return jnp.einsum("bqk,bke->bqe", attn_probs.astype(jnp.float32), values_all.astype(jnp.float32)).astype(jnp.bfloat16)


def layer_step(resid, params):
    ln1_gain, ln1_bias, ln2_gain, ln2_bias, w_qkv, w_out, b_out, w_up, b_up, w_down, b_down = params
    normed = layer_norm(resid, ln1_gain, ln1_bias)
    qkv_proj = jnp.dot(normed.reshape(BATCH * SEQ_LEN, D_MODEL), w_qkv.reshape(D_MODEL, 3 * HEADS * HEAD_DIM), preferred_element_type=jnp.float32).astype(jnp.bfloat16)
    qkv_proj = qkv_proj.reshape(BATCH, SEQ_LEN, 3, HEADS, HEAD_DIM)
    heads_first = jnp.transpose(qkv_proj, (2, 3, 0, 1, 4))
    attn_heads = lax.map(attention_head, (heads_first[0], heads_first[1], heads_first[2]))
    attn_out = jnp.einsum("hbse,hed->bsd", attn_heads.astype(jnp.float32), w_out.astype(jnp.float32))
    resid = resid + (attn_out + b_out)
    normed_mlp = layer_norm(resid, ln2_gain, ln2_bias)
    pre_act = jnp.dot(normed_mlp.reshape(BATCH * SEQ_LEN, D_MODEL), w_up, preferred_element_type=jnp.float32) + b_up
    hidden = jax.nn.gelu(pre_act, approximate=True).astype(jnp.bfloat16)
    mlp_out = jnp.dot(hidden, w_down, preferred_element_type=jnp.float32).reshape(BATCH, SEQ_LEN, D_MODEL)
    resid = resid + (mlp_out + b_down)
    return resid, None


def reference(x_tokens, ln1_gain, ln1_bias, ln2_gain, ln2_bias, w_qkv, w_out, b_out, w_up, b_up, w_down, b_down):
    params = (ln1_gain, ln1_bias, ln2_gain, ln2_bias, w_qkv, w_out, b_out, w_up, b_up, w_down, b_down)
    resid, _ = lax.scan(layer_step, x_tokens.astype(jnp.float32), params)
    return resid.astype(jnp.bfloat16)
```

```python
import functools
import math
import jax
import jax.numpy as jnp
from jax import lax
from jax.experimental import pallas as pl
from jax.experimental.pallas import tpu as pltpu
from jax.sharding import PartitionSpec as P


def layer_norm(resid, gain, shift):
    row_mean = jnp.mean(resid, axis=-1, keepdims=True)
    centered = resid - row_mean
    variance = jnp.mean(centered * centered, axis=-1, keepdims=True)
    return (centered * lax.rsqrt(variance + 1e-5) * gain + shift).astype(jnp.bfloat16)


def attention_body(heads, scale, q_ref, k_ref, v_ref, o_ref):
    seq = q_ref.shape[0]
    block = 256
    for head in range(heads):
        cols = slice(head * 128, (head + 1) * 128)
        for start in range(0, seq, block):
            stop = start + block
            scores = lax.dot_general(q_ref[start:stop, cols], k_ref[0:stop, cols], (((1,), (1,)), ((), ())),
                                     preferred_element_type=jnp.float32) * scale
            rows = lax.broadcasted_iota(jnp.int32, scores.shape, 0) + start
            keys = lax.broadcasted_iota(jnp.int32, scores.shape, 1)
            scores = jnp.where(rows >= keys, scores, -1e30)
            top = jnp.max(scores, axis=-1, keepdims=True)
            weights = jnp.exp(scores - top)
            probs = (weights / jnp.sum(weights, axis=-1, keepdims=True)).astype(jnp.bfloat16)
            o_ref[start:stop, cols] = jnp.dot(probs, v_ref[0:stop, cols], preferred_element_type=jnp.float32).astype(jnp.bfloat16)


def attention(qkv, heads):
    seq = qkv.shape[0]
    per_step = 4
    steps = heads // per_step
    width = per_step * 128
    specs = [pl.BlockSpec((seq, width), functools.partial(lambda t, g: (0, t * steps + g), t)) for t in range(3)]
    return pl.pallas_call(
        functools.partial(attention_body, per_step, 1.0 / math.sqrt(128)),
        grid=(steps,),
        in_specs=specs,
        out_specs=pl.BlockSpec((seq, width), lambda g: (0, g)),
        out_shape=jax.ShapeDtypeStruct((seq, heads * 128), jnp.bfloat16),
        cost_estimate=pl.CostEstimate(flops=60 * seq * seq * heads * 128, bytes_accessed=8 * seq * heads * 128, transcendentals=seq * seq * heads),
    )(qkv, qkv, qkv)


def solution(mesh):
    across = [(i, i ^ 2) for i in range(4)]
    beside = [(i, i ^ 1) for i in range(4)]

    def swap_x(value):
        return lax.ppermute(value, "tp", across)

    def swap_core(value):
        return lax.ppermute(value, "tp", beside)

    def local_forward(x_local, ln1_gain, ln1_bias, ln2_gain, ln2_bias, w_qkv, w_out, b_out, w_up, b_up, w_down, b_down):
        batch, rows, width = x_local.shape
        layers = w_qkv.shape[0]
        heads = w_qkv.shape[3]
        seq = rows * 4
        mine = batch // 2
        me = lax.axis_index("tp")
        core = me % 2
        chip = me // 2

        x_pairs = x_local.reshape(2, mine, rows, width)
        tokens = []
        for j in range(mine):
            gathered = lax.all_gather(x_pairs[:, j], "tp", axis=1, tiled=True)
            tokens.append(lax.dynamic_index_in_dim(gathered, core, 0, keepdims=False))

        qkv_flat = [w_qkv[l].reshape(width, 3 * heads * 128) for l in range(layers)]
        out_flat = [w_out[l].reshape(heads * 128, width) for l in range(layers)]
        weights = []
        b_up_other = swap_core(b_up)
        for l in range(layers):
            own = (qkv_flat[l], out_flat[l], w_up[l], w_down[l])
            other = tuple(swap_core(w) for w in own)
            weights.append((own, other))

        previous = None

        def gate(*values):
            return values if previous is None else lax.optimization_barrier((*values, previous))[:-1]

        state = [(t,) for t in tokens]
        finals = []
        for l in range(layers):
            for j in range(mine):
                if l == 0:
                    (token,) = gate(*state[j])
                    resid = token.astype(jnp.float32)
                else:
                    resid, kept, got = gate(*state[j])
                    resid = resid + ((kept + got.astype(jnp.float32)) + b_down[l - 1])
                (qkv_a, out_a, up_a, down_a), (qkv_b, out_b, up_b, down_b) = weights[l]
                normed = layer_norm(resid, ln1_gain[l], ln1_bias[l])
                qa = jnp.dot(normed, qkv_a, preferred_element_type=jnp.float32).astype(jnp.bfloat16)
                oa = attention(qa, heads)
                qb = jnp.dot(normed, qkv_b, preferred_element_type=jnp.float32).astype(jnp.bfloat16)
                ob = attention(qb, heads)
                partial = jnp.dot(oa, out_a, preferred_element_type=jnp.float32) + jnp.dot(ob, out_b, preferred_element_type=jnp.float32)
                narrow = partial.astype(jnp.bfloat16)
                state[j] = (resid, partial, swap_x(narrow))
                previous = narrow
            for j in range(mine):
                resid, kept, got = gate(*state[j])
                resid = resid + ((kept + got.astype(jnp.float32)) + b_out[l])
                normed = layer_norm(resid, ln2_gain[l], ln2_bias[l])
                (qkv_a, out_a, up_a, down_a), (qkv_b, out_b, up_b, down_b) = weights[l]
                ua = jax.nn.gelu(jnp.dot(normed, up_a, preferred_element_type=jnp.float32) + b_up[l], approximate=True).astype(jnp.bfloat16)
                ub = jax.nn.gelu(jnp.dot(normed, up_b, preferred_element_type=jnp.float32) + b_up_other[l], approximate=True).astype(jnp.bfloat16)
                partial = jnp.dot(ua, down_a, preferred_element_type=jnp.float32) + jnp.dot(ub, down_b, preferred_element_type=jnp.float32)
                narrow = partial.astype(jnp.bfloat16)
                previous = narrow
                if l < layers - 1:
                    state[j] = (resid, partial, swap_x(narrow))
                    if j == 0:
                        held = gate(*weights[l + 1][1])
                        weights[l + 1] = (weights[l + 1][0], held)
                        previous = lax.optimization_barrier((previous, *held))[0]
                else:
                    half = seq // 2
                    got = swap_x(lax.dynamic_slice_in_dim(narrow, (1 - chip) * half, half, 0))
                    own = lax.dynamic_slice_in_dim(partial, chip * half, half, 0)
                    r = lax.dynamic_slice_in_dim(resid, chip * half, half, 0)
                    state[j] = (r, own, got)
        for j in range(mine):
            r, own, got = gate(*state[j]) if j < mine - 1 else state[j]
            done = (r + ((own + got.astype(jnp.float32)) + b_down[layers - 1])).astype(jnp.bfloat16).reshape(2, rows, width)
            stay = lax.dynamic_index_in_dim(done, core, 0, keepdims=False)
            go = swap_core(lax.dynamic_index_in_dim(done, 1 - core, 0, keepdims=False))
            finals.append((stay, go))
        first = jnp.stack([jnp.where(core == 0, s, g) for s, g in finals])
        second = jnp.stack([jnp.where(core == 0, g, s) for s, g in finals])
        return jnp.concatenate([first, second], axis=0)

    rows_spec = P("dp", "tp", None)
    in_specs = (rows_spec, P(), P(), P(), P(), P(None, None, None, "tp", None), P(None, "tp", None, None), P(), P(None, None, "tp"), P(None, "tp"), P(None, "tp", None), P())
    return jax.shard_map(local_forward, mesh=mesh, in_specs=in_specs, out_specs=rows_spec, check_vma=False)
```

```python
import functools
import math
import jax
import jax.numpy as jnp
from jax import lax
from jax.experimental import pallas as pl
from jax.experimental.pallas import tpu as pltpu
from jax.sharding import PartitionSpec as P


SEQ = 512
WIDTH = 4096
HEAD = 128
TILE = 512
CHUNK = 64
CHUNKS = SEQ // CHUNK
VMEM_LIMIT = 60 * 1024 * 1024


def norm_chunk(first, i, res, nar, gain, shift):
    rows = pl.ds(pl.multiple_of(i * CHUNK, CHUNK), CHUNK)
    total = jnp.zeros((CHUNK, 128), jnp.float32)
    for t in range(WIDTH // 128):
        cols = slice(t * 128, (t + 1) * 128)
        value = nar[rows, cols].astype(jnp.float32)
        if not first:
            value = res[rows, cols] + value
        res[rows, cols] = value
        total = total + value
    mean = jnp.sum(total, axis=-1, keepdims=True) * (1.0 / WIDTH)
    total = jnp.zeros((CHUNK, 128), jnp.float32)
    for t in range(WIDTH // 128):
        centered = res[rows, t * 128:(t + 1) * 128] - mean
        total = total + centered * centered
    inv = lax.rsqrt(jnp.sum(total, axis=-1, keepdims=True) * (1.0 / WIDTH) + 1e-5)
    for t in range(WIDTH // 128):
        cols = slice(t * 128, (t + 1) * 128)
        nar[rows, cols] = ((res[rows, cols] - mean) * inv * gain[0:1, cols] + shift[0:1, cols]).astype(jnp.bfloat16)


def load_and_norm(first, idx, source, res, nar, gain, shift, sems):
    def copies(i):
        rows = pl.ds(pl.multiple_of(i * CHUNK, CHUNK), CHUNK)
        if first:
            return [pltpu.make_async_copy(source[0].at[idx[0], rows], nar.at[rows], sems.at[0, i])]
        return [pltpu.make_async_copy(source[0].at[rows], res.at[rows], sems.at[0, i]),
                pltpu.make_async_copy(source[1].at[rows], nar.at[rows], sems.at[1, i])]

    def start():
        for i in range(CHUNKS):
            for c in copies(i):
                c.start()

    def finish():
        @pl.loop(0, CHUNKS)
        def _(i):
            for c in copies(i):
                c.wait()
            norm_chunk(first, i, res, nar, gain, shift)

    return start, finish


def head_attention(scale, qkv, slot, out, base):
    block = 256
    for head in range(2):
        cols = slice(head * HEAD, (head + 1) * HEAD)
        for start in range(0, SEQ, block):
            stop = start + block
            q = qkv[slot, 0, start:stop, cols]
            k = qkv[slot, 1, 0:stop, cols]
            v = qkv[slot, 2, 0:stop, cols]
            scores = lax.dot_general(q, k, (((1,), (1,)), ((), ())), preferred_element_type=jnp.float32) * scale
            rows = lax.broadcasted_iota(jnp.int32, scores.shape, 0) + start
            keys = lax.broadcasted_iota(jnp.int32, scores.shape, 1)
            scores = jnp.where(rows >= keys, scores, -1e30)
            top = jnp.max(scores, axis=-1, keepdims=True)
            weights = jnp.exp(scores - top)
            probs = (weights / jnp.sum(weights, axis=-1, keepdims=True)).astype(jnp.bfloat16)
            result = jnp.dot(probs, v, preferred_element_type=jnp.float32).astype(jnp.bfloat16)
            out[start:stop, pl.ds(pl.multiple_of(base + head * HEAD, HEAD), HEAD)] = result


def attention_stage(layer, first, heads, *refs):
    sources, refs = refs[1:2 if first else 3], (refs[0],) + refs[2 if first else 3:]
    (idx, gain, shift, bias, wq_own, wq_par, wo_own, wo_par, send, keep,
     res, nar, out, qkv, wq, wo, stage, load_sems, wq_sems, wo_sems, out_sems) = refs
    scale = 1.0 / math.sqrt(HEAD)
    per_kind = heads * HEAD
    groups = heads // 2
    start_load, finish_load = load_and_norm(first, idx, sources, res, nar, gain, shift, load_sems)

    def wq_copies(g, own, local=None):
        slot = lax.rem(g, 2)
        source = wq_own if own else wq_par
        if local is None:
            local = g if own else g - groups
        return [pltpu.make_async_copy(source.at[:, pl.ds(pl.multiple_of(t * per_kind + local * 256, 256), 256)], wq.at[slot, t], wq_sems.at[slot])
                for t in range(3)]

    def start_wq(g):
        @pl.when(g < groups)
        def _():
            for c in wq_copies(g, True):
                c.start()

        @pl.when((g >= groups) & (g < 2 * groups))
        def _():
            for c in wq_copies(g, False):
                c.start()

    def wo_copies(n):
        slot = lax.rem(n, 3)
        cols = pl.ds(pl.multiple_of(n * TILE, TILE), TILE)
        return [pltpu.make_async_copy(w.at[layer, :, cols], wo.at[slot, s], wo_sems.at[slot]) for s, w in enumerate((wo_own, wo_par))]

    def project(g):
        slot = lax.rem(g, 2)
        for c in wq_copies(g, True, 0):
            c.wait()
        for t in range(3):
            qkv[slot, t] = jnp.dot(nar[...], wq[slot, t], preferred_element_type=jnp.float32).astype(jnp.bfloat16)

    for c in wq_copies(0, True):
        c.start()
    start_load()
    for c in wq_copies(1, True):
        c.start()
    for n in range(2):
        for c in wo_copies(n):
            c.start()
    finish_load()
    project(0)

    @pl.loop(1, 2 * groups)
    def _(g):
        start_wq(g + 1)
        head_attention(scale, qkv, lax.rem(g - 1, 2), out, (g - 1) * 256)
        project(g)

    head_attention(scale, qkv, (2 * groups - 1) % 2, out, (2 * groups - 1) * 256)

    def out_copies(n):
        cols = pl.ds(pl.multiple_of(n * TILE, TILE), TILE)
        slot = lax.rem(n, 2)
        return [pltpu.make_async_copy(stage.at[slot], send.at[:, cols], out_sems.at[0, slot]),
                pltpu.make_async_copy(res.at[:, cols], keep.at[:, cols], out_sems.at[1, slot])]

    steps = WIDTH // TILE

    @pl.loop(0, steps)
    def _(n):
        slot = lax.rem(n, 3)
        cols = pl.ds(pl.multiple_of(n * TILE, TILE), TILE)

        @pl.when(n + 2 < steps)
        def _():
            for c in wo_copies(n + 2):
                c.start()

        for c in wo_copies(n):
            c.wait()

        @pl.when(n >= 2)
        def _():
            for c in out_copies(n - 2):
                c.wait()

        part = jnp.dot(out[:, :per_kind], wo[slot, 0], preferred_element_type=jnp.float32)
        part = part + jnp.dot(out[:, per_kind:], wo[slot, 1], preferred_element_type=jnp.float32)
        stage[lax.rem(n, 2)] = part.astype(jnp.bfloat16)
        res[:, cols] = res[:, cols] + (part + bias[0:1, cols])
        for c in out_copies(n):
            c.start()

    for n in (steps - 2, steps - 1):
        for c in out_copies(n):
            c.wait()


def mlp_stage(layer, last, idx, kept, got, gain, shift, bias_up, bias, up_own, up_par, down_own, down_par, send, keep,
              res, nar, hidden, ring, stage, load_sems, ring_sems, out_sems):
    start_load, finish_load = load_and_norm(False, idx, (kept, got), res, nar, gain, shift, load_sems)
    half_tiles = up_own.shape[2] // TILE
    ups = 2 * half_tiles
    steps = WIDTH // TILE

    def tile_copy(i, source, n):
        slot = lax.rem(i, 4)
        cols = pl.ds(pl.multiple_of(n * TILE, TILE), TILE)
        return pltpu.make_async_copy(source.at[layer, :, cols], ring.at[slot], ring_sems.at[slot])

    def start_up(i):
        @pl.when(i < half_tiles)
        def _():
            tile_copy(i, up_own, i).start()

        @pl.when((i >= half_tiles) & (i < ups))
        def _():
            tile_copy(i, up_par, i - half_tiles).start()

        @pl.when(i >= ups)
        def _():
            start_down(i)

    def start_down(i):
        j = i - ups

        @pl.when((lax.rem(j, 2) == 0) & (j < 2 * steps))
        def _():
            tile_copy(i, down_own, j // 2).start()

        @pl.when((lax.rem(j, 2) == 1) & (j < 2 * steps))
        def _():
            tile_copy(i, down_par, j // 2).start()

    tile_copy(0, up_own, 0).start()
    start_load()
    tile_copy(1, up_own, 1).start()
    tile_copy(2, up_own, 2).start()
    finish_load()

    @pl.loop(0, ups)
    def _(i):
        start_up(i + 3)
        tile_copy(i, up_own, 0).wait()
        t = jnp.dot(nar[...], ring[lax.rem(i, 4)], preferred_element_type=jnp.float32) + bias_up[i]
        u = 0.5 * t * (1.0 + jnp.tanh(math.sqrt(2.0 / math.pi) * (t + 0.044715 * (t * t * t))))
        part = i // half_tiles
        hidden[part, :, pl.ds(pl.multiple_of((i - part * half_tiles) * TILE, TILE), TILE)] = u.astype(jnp.bfloat16)

    half = SEQ // 2

    def out_copies(n):
        cols = pl.ds(pl.multiple_of(n * TILE, TILE), TILE)
        slot = lax.rem(n, 2)
        if last:
            chip = idx[1]
            theirs = pl.ds(pl.multiple_of((1 - chip) * half, half), half)
            ours = pl.ds(pl.multiple_of(chip * half, half), half)
            return [pltpu.make_async_copy(stage.at[slot, theirs], send.at[:, cols], out_sems.at[0, slot]),
                    pltpu.make_async_copy(res.at[ours, cols], keep.at[:, cols], out_sems.at[1, slot])]
        return [pltpu.make_async_copy(stage.at[slot], send.at[:, cols], out_sems.at[0, slot]),
                pltpu.make_async_copy(res.at[:, cols], keep.at[:, cols], out_sems.at[1, slot])]

    @pl.loop(0, steps)
    def _(n):
        i = ups + 2 * n
        cols = pl.ds(pl.multiple_of(n * TILE, TILE), TILE)

        @pl.when(n > 0)
        def _():
            start_down(i + 2)

        start_down(i + 3)
        tile_copy(i, down_own, 0).wait()
        tile_copy(i + 1, down_own, 0).wait()

        @pl.when(n >= 2)
        def _():
            for c in out_copies(n - 2):
                c.wait()

        part = jnp.dot(hidden[0], ring[lax.rem(i, 4)], preferred_element_type=jnp.float32)
        part = part + jnp.dot(hidden[1], ring[lax.rem(i + 1, 4)], preferred_element_type=jnp.float32)
        stage[lax.rem(n, 2)] = part.astype(jnp.bfloat16)
        res[:, cols] = res[:, cols] + (part + bias[0:1, cols])
        for c in out_copies(n):
            c.start()

    for n in (steps - 2, steps - 1):
        for c in out_copies(n):
            c.wait()


ANY = pl.BlockSpec(memory_space=pl.ANY)
VMEM = pl.BlockSpec(memory_space=pltpu.VMEM)
SMEM = pl.BlockSpec(memory_space=pltpu.SMEM)


def run_attention(layer, first, heads, idx, sources, gain, shift, bias, wq_own, wq_par, wo_own, wo_par):
    flops = 2 * SEQ * WIDTH * heads * HEAD * 8 + 8 * SEQ * SEQ * heads * HEAD
    return pl.pallas_call(
        functools.partial(attention_stage, layer, first, heads),
        in_specs=[SMEM] + [ANY] * len(sources) + [VMEM] * 3 + [ANY] * 4,
        out_specs=[ANY, ANY],
        out_shape=[jax.ShapeDtypeStruct((SEQ, WIDTH), jnp.bfloat16), jax.ShapeDtypeStruct((SEQ, WIDTH), jnp.float32)],
        scratch_shapes=[
            pltpu.VMEM((SEQ, WIDTH), jnp.float32),
            pltpu.VMEM((SEQ, WIDTH), jnp.bfloat16),
            pltpu.VMEM((SEQ, 2 * heads * HEAD), jnp.bfloat16),
            pltpu.VMEM((2, 3, SEQ, 256), jnp.bfloat16),
            pltpu.VMEM((2, 3, WIDTH, 256), jnp.bfloat16),
            pltpu.VMEM((3, 2, heads * HEAD, TILE), jnp.bfloat16),
            pltpu.VMEM((2, SEQ, TILE), jnp.bfloat16),
            pltpu.SemaphoreType.DMA((2, CHUNKS)),
            pltpu.SemaphoreType.DMA((2,)),
            pltpu.SemaphoreType.DMA((3,)),
            pltpu.SemaphoreType.DMA((2, 2)),
        ],
        compiler_params=pltpu.CompilerParams(vmem_limit_bytes=VMEM_LIMIT),
        cost_estimate=pl.CostEstimate(flops=flops, bytes_accessed=100_000_000, transcendentals=SEQ * SEQ * heads * 2),
    )(idx, *sources, gain, shift, bias, wq_own, wq_par, wo_own, wo_par)


def run_mlp(layer, last, idx, kept, got, gain, shift, bias_up, bias, up_own, up_par, down_own, down_par):
    rows = SEQ // 2 if last else SEQ
    flops = 8 * SEQ * WIDTH * up_own.shape[2]
    return pl.pallas_call(
        functools.partial(mlp_stage, layer, last),
        in_specs=[SMEM] + [ANY] * 2 + [VMEM] * 4 + [ANY] * 4,
        out_specs=[ANY, ANY],
        out_shape=[jax.ShapeDtypeStruct((rows, WIDTH), jnp.bfloat16), jax.ShapeDtypeStruct((rows, WIDTH), jnp.float32)],
        scratch_shapes=[
            pltpu.VMEM((SEQ, WIDTH), jnp.float32),
            pltpu.VMEM((SEQ, WIDTH), jnp.bfloat16),
            pltpu.VMEM((2, SEQ, up_own.shape[2]), jnp.bfloat16),
            pltpu.VMEM((4, WIDTH, TILE), jnp.bfloat16),
            pltpu.VMEM((2, SEQ, TILE), jnp.bfloat16),
            pltpu.SemaphoreType.DMA((2, CHUNKS)),
            pltpu.SemaphoreType.DMA((4,)),
            pltpu.SemaphoreType.DMA((2, 2)),
        ],
        compiler_params=pltpu.CompilerParams(vmem_limit_bytes=VMEM_LIMIT),
        cost_estimate=pl.CostEstimate(flops=flops, bytes_accessed=160_000_000, transcendentals=2 * SEQ * up_own.shape[2]),
    )(idx, kept, got, gain, shift, bias_up, bias, up_own, up_par, down_own, down_par)


ORDER = ([("a", 0, j) for j in range(4)] + [("m", 0, j) for j in range(4)]
         + [("a", 1, j) for j in range(4)] + [("m", 1, j) for j in range(4)])


def solution(mesh):
    across = [(i, i ^ 2) for i in range(4)]
    beside = [(i, i ^ 1) for i in range(4)]

    def swap_core(value):
        return lax.ppermute(value, "tp", beside)

    def body(x_local, ln1_gain, ln1_bias, ln2_gain, ln2_bias, w_qkv, w_out, b_out, w_up, b_up, w_down, b_down):
        batch, rows, width = x_local.shape
        layers = w_qkv.shape[0]
        heads = w_qkv.shape[3]
        mine = batch // 2
        me = lax.axis_index("tp")
        core = lax.rem(me, 2)
        chip = me // 2
        idx = jnp.stack([core, chip]).astype(jnp.int32)

        x_pairs = x_local.reshape(2, mine, rows, width)
        tokens = [lax.all_gather(x_pairs[:, j], "tp", axis=1, tiled=True) for j in range(mine)]

        out_own = w_out.reshape(layers, heads * HEAD, width)
        qkv_own, qkv_par = [], []
        for l in range(layers):
            qkv_own.append(w_qkv[l].reshape(width, 3 * heads * HEAD))
            qkv_par.append(swap_core(qkv_own[l]))
        out_par = swap_core(out_own)
        up_par = swap_core(w_up)
        down_par = swap_core(w_down)
        up_bias = jnp.stack([b_up, swap_core(b_up)], axis=1).reshape(layers, -1, 1, TILE)

        state = [None] * mine
        finals = [None] * mine
        for kind, l, j in ORDER:
            last = l == layers - 1
            if kind == "a":
                sources = (tokens[j],) if l == 0 else state[j]
                send, keep = run_attention(l, l == 0, heads, idx, sources, ln1_gain[l:l + 1], ln1_bias[l:l + 1], b_out[l:l + 1],
                                           qkv_own[l], qkv_par[l], out_own, out_par)
            else:
                send, keep = run_mlp(l, last, idx, *state[j], ln2_gain[l:l + 1], ln2_bias[l:l + 1], up_bias[l], b_down[l:l + 1],
                                     w_up, up_par, w_down, down_par)
            got = lax.ppermute(send, "tp", across)
            state[j] = (keep, got)
            if kind == "m" and last:
                done = (keep + got.astype(jnp.float32)).astype(jnp.bfloat16).reshape(2, rows, width)
                stay = lax.dynamic_index_in_dim(done, core, 0, keepdims=False)
                go = swap_core(lax.dynamic_index_in_dim(done, 1 - core, 0, keepdims=False))
                finals[j] = (stay, go)
        first = jnp.stack([jnp.where(core == 0, s, g) for s, g in finals])
        second = jnp.stack([jnp.where(core == 0, g, s) for s, g in finals])
        return jnp.concatenate([first, second], axis=0)


    rows_spec = P("dp", "tp", None)
    in_specs = (rows_spec, P(), P(), P(), P(), P(None, None, None, "tp", None), P(None, "tp", None, None), P(), P(None, None, "tp"), P(None, "tp"), P(None, "tp", None), P())
    return jax.shard_map(body, mesh=mesh, in_specs=in_specs, out_specs=rows_spec, check_vma=False)
```

```python
import functools
import math
import jax
import jax.numpy as jnp
from jax import lax
from jax.experimental import pallas as pl
from jax.experimental.pallas import tpu as pltpu
from jax.sharding import PartitionSpec as P


SEQ = 512
WIDTH = 4096
HEAD = 128
TILE = 512
CHUNK = 64
CHUNKS = SEQ // CHUNK
VMEM_LIMIT = 60 * 1024 * 1024


def norm_chunk(first, i, res, nar, gain, shift):
    rows = pl.ds(pl.multiple_of(i * CHUNK, CHUNK), CHUNK)
    total = jnp.zeros((CHUNK, 128), jnp.float32)
    for t in range(WIDTH // 128):
        cols = slice(t * 128, (t + 1) * 128)
        value = nar[rows, cols].astype(jnp.float32)
        if not first:
            value = res[rows, cols] + value
        res[rows, cols] = value
        total = total + value
    mean = jnp.sum(total, axis=-1, keepdims=True) * (1.0 / WIDTH)
    total = jnp.zeros((CHUNK, 128), jnp.float32)
    for t in range(WIDTH // 128):
        centered = res[rows, t * 128:(t + 1) * 128] - mean
        total = total + centered * centered
    inv = lax.rsqrt(jnp.sum(total, axis=-1, keepdims=True) * (1.0 / WIDTH) + 1e-5)
    for t in range(WIDTH // 128):
        cols = slice(t * 128, (t + 1) * 128)
        nar[rows, cols] = ((res[rows, cols] - mean) * inv * gain[0:1, cols] + shift[0:1, cols]).astype(jnp.bfloat16)


def load_and_norm(first, idx, source, res, nar, gain, shift, sems):
    def copies(i):
        rows = pl.ds(pl.multiple_of(i * CHUNK, CHUNK), CHUNK)
        if first:
            return [pltpu.make_async_copy(source[0].at[idx[0], rows], nar.at[rows], sems.at[0, i])]
        return [pltpu.make_async_copy(source[0].at[rows], res.at[rows], sems.at[0, i]),
                pltpu.make_async_copy(source[1].at[rows], nar.at[rows], sems.at[1, i])]

    def start():
        for i in range(CHUNKS):
            for c in copies(i):
                c.start()

    def finish():
        @pl.loop(0, CHUNKS)
        def _(i):
            for c in copies(i):
                c.wait()
            norm_chunk(first, i, res, nar, gain, shift)

    return start, finish


def head_attention(scale, qkv, slot, out, base):
    block = 256
    for head in range(2):
        cols = slice(head * HEAD, (head + 1) * HEAD)
        for start in range(0, SEQ, block):
            stop = start + block
            q = qkv[slot, 0, start:stop, cols]
            k = qkv[slot, 1, 0:stop, cols]
            v = qkv[slot, 2, 0:stop, cols]
            scores = lax.dot_general(q, k, (((1,), (1,)), ((), ())), preferred_element_type=jnp.float32) * scale
            rows = lax.broadcasted_iota(jnp.int32, scores.shape, 0) + start
            keys = lax.broadcasted_iota(jnp.int32, scores.shape, 1)
            scores = jnp.where(rows >= keys, scores, -1e30)
            top = jnp.max(scores, axis=-1, keepdims=True)
            weights = jnp.exp(scores - top)
            probs = (weights / jnp.sum(weights, axis=-1, keepdims=True)).astype(jnp.bfloat16)
            result = jnp.dot(probs, v, preferred_element_type=jnp.float32).astype(jnp.bfloat16)
            out[start:stop, pl.ds(pl.multiple_of(base + head * HEAD, HEAD), HEAD)] = result


def attention_stage(layer, first, heads, *refs):
    sources, refs = refs[1:2 if first else 3], (refs[0],) + refs[2 if first else 3:]
    (idx, gain, shift, bias, wq_own, wq_par, wo_own, wo_par, send, keep,
     res, nar, out, qkv, wq, wo, stage, load_sems, wq_sems, wo_sems, out_sems) = refs
    scale = 1.0 / math.sqrt(HEAD)
    per_kind = heads * HEAD
    groups = heads // 2
    start_load, finish_load = load_and_norm(first, idx, sources, res, nar, gain, shift, load_sems)

    def wq_copies(g, own, local=None):
        slot = lax.rem(g, 2)
        source = wq_own if own else wq_par
        if local is None:
            local = g if own else g - groups
        return [pltpu.make_async_copy(source.at[:, pl.ds(pl.multiple_of(t * per_kind + local * 256, 256), 256)], wq.at[slot, t], wq_sems.at[slot])
                for t in range(3)]

    def start_wq(g):
        @pl.when(g < groups)
        def _():
            for c in wq_copies(g, True):
                c.start()

        @pl.when((g >= groups) & (g < 2 * groups))
        def _():
            for c in wq_copies(g, False):
                c.start()

    def wo_copies(n):
        slot = lax.rem(n, 3)
        cols = pl.ds(pl.multiple_of(n * TILE, TILE), TILE)
        return [pltpu.make_async_copy(w.at[layer, :, cols], wo.at[slot, s], wo_sems.at[slot]) for s, w in enumerate((wo_own, wo_par))]

    def project(g):
        slot = lax.rem(g, 2)
        for c in wq_copies(g, True, 0):
            c.wait()
        for t in range(3):
            qkv[slot, t] = jnp.dot(nar[...], wq[slot, t], preferred_element_type=jnp.float32).astype(jnp.bfloat16)

    for c in wq_copies(0, True):
        c.start()
    start_load()
    for c in wq_copies(1, True):
        c.start()
    for n in range(2):
        for c in wo_copies(n):
            c.start()
    finish_load()
    project(0)

    @pl.loop(1, 2 * groups)
    def _(g):
        start_wq(g + 1)
        head_attention(scale, qkv, lax.rem(g - 1, 2), out, (g - 1) * 256)
        project(g)

    head_attention(scale, qkv, (2 * groups - 1) % 2, out, (2 * groups - 1) * 256)

    def out_copies(n):
        cols = pl.ds(pl.multiple_of(n * TILE, TILE), TILE)
        slot = lax.rem(n, 2)
        return [pltpu.make_async_copy(stage.at[slot], send.at[:, cols], out_sems.at[0, slot]),
                pltpu.make_async_copy(res.at[:, cols], keep.at[:, cols], out_sems.at[1, slot])]

    steps = WIDTH // TILE

    @pl.loop(0, steps)
    def _(n):
        slot = lax.rem(n, 3)
        cols = pl.ds(pl.multiple_of(n * TILE, TILE), TILE)

        @pl.when(n + 2 < steps)
        def _():
            for c in wo_copies(n + 2):
                c.start()

        for c in wo_copies(n):
            c.wait()

        @pl.when(n >= 2)
        def _():
            for c in out_copies(n - 2):
                c.wait()

        part = jnp.dot(out[:, :per_kind], wo[slot, 0], preferred_element_type=jnp.float32)
        part = part + jnp.dot(out[:, per_kind:], wo[slot, 1], preferred_element_type=jnp.float32)
        stage[lax.rem(n, 2)] = part.astype(jnp.bfloat16)
        res[:, cols] = res[:, cols] + (part + bias[0:1, cols])
        for c in out_copies(n):
            c.start()

    for n in (steps - 2, steps - 1):
        for c in out_copies(n):
            c.wait()


def mlp_stage(layer, last, idx, kept, got, gain, shift, bias_up, bias, up_own, up_par, down_own, down_par, send, keep,
              res, nar, hidden, ring, stage, load_sems, ring_sems, out_sems):
    start_load, finish_load = load_and_norm(False, idx, (kept, got), res, nar, gain, shift, load_sems)
    half_tiles = up_own.shape[2] // TILE
    ups = 2 * half_tiles
    steps = WIDTH // TILE

    def tile_copy(i, source, n):
        slot = lax.rem(i, 4)
        cols = pl.ds(pl.multiple_of(n * TILE, TILE), TILE)
        return pltpu.make_async_copy(source.at[layer, :, cols], ring.at[slot], ring_sems.at[slot])

    def start_up(i):
        @pl.when(i < half_tiles)
        def _():
            tile_copy(i, up_own, i).start()

        @pl.when((i >= half_tiles) & (i < ups))
        def _():
            tile_copy(i, up_par, i - half_tiles).start()

        @pl.when(i >= ups)
        def _():
            start_down(i)

    def start_down(i):
        j = i - ups

        @pl.when((lax.rem(j, 2) == 0) & (j < 2 * steps))
        def _():
            tile_copy(i, down_own, j // 2).start()

        @pl.when((lax.rem(j, 2) == 1) & (j < 2 * steps))
        def _():
            tile_copy(i, down_par, j // 2).start()

    tile_copy(0, up_own, 0).start()
    start_load()
    tile_copy(1, up_own, 1).start()
    tile_copy(2, up_own, 2).start()
    finish_load()

    @pl.loop(0, ups)
    def _(i):
        start_up(i + 3)
        tile_copy(i, up_own, 0).wait()
        t = jnp.dot(nar[...], ring[lax.rem(i, 4)], preferred_element_type=jnp.float32) + bias_up[i]
        u = 0.5 * t * (1.0 + jnp.tanh(math.sqrt(2.0 / math.pi) * (t + 0.044715 * (t * t * t))))
        part = i // half_tiles
        hidden[part, :, pl.ds(pl.multiple_of((i - part * half_tiles) * TILE, TILE), TILE)] = u.astype(jnp.bfloat16)

    half = SEQ // 2

    def out_copies(n):
        cols = pl.ds(pl.multiple_of(n * TILE, TILE), TILE)
        slot = lax.rem(n, 2)
        if last:
            chip = idx[1]
            theirs = pl.ds(pl.multiple_of((1 - chip) * half, half), half)
            ours = pl.ds(pl.multiple_of(chip * half, half), half)
            return [pltpu.make_async_copy(stage.at[slot, theirs], send.at[:, cols], out_sems.at[0, slot]),
                    pltpu.make_async_copy(res.at[ours, cols], keep.at[:, cols], out_sems.at[1, slot])]
        return [pltpu.make_async_copy(stage.at[slot], send.at[:, cols], out_sems.at[0, slot]),
                pltpu.make_async_copy(res.at[:, cols], keep.at[:, cols], out_sems.at[1, slot])]

    @pl.loop(0, steps)
    def _(n):
        i = ups + 2 * n
        cols = pl.ds(pl.multiple_of(n * TILE, TILE), TILE)

        @pl.when(n > 0)
        def _():
            start_down(i + 2)

        start_down(i + 3)
        tile_copy(i, down_own, 0).wait()
        tile_copy(i + 1, down_own, 0).wait()

        @pl.when(n >= 2)
        def _():
            for c in out_copies(n - 2):
                c.wait()

        part = jnp.dot(hidden[0], ring[lax.rem(i, 4)], preferred_element_type=jnp.float32)
        part = part + jnp.dot(hidden[1], ring[lax.rem(i + 1, 4)], preferred_element_type=jnp.float32)
        stage[lax.rem(n, 2)] = part.astype(jnp.bfloat16)
        res[:, cols] = res[:, cols] + (part + bias[0:1, cols])
        for c in out_copies(n):
            c.start()

    for n in (steps - 2, steps - 1):
        for c in out_copies(n):
            c.wait()


def flatten_heads(w_ref, out_ref):
    _, rows, kinds, heads, _ = w_ref.shape
    for kind in range(kinds):
        out_ref[:, kind * heads * HEAD:(kind + 1) * heads * HEAD] = w_ref[0, :, kind].reshape(rows, heads * HEAD)


def run_flatten(layer, w_qkv):
    _, width, kinds, heads, _ = w_qkv.shape
    rows = 256
    return pl.pallas_call(
        flatten_heads,
        grid=(width // rows,),
        in_specs=[pl.BlockSpec((1, rows, kinds, heads, HEAD), lambda i: (layer, i, 0, 0, 0))],
        out_specs=pl.BlockSpec((rows, kinds * heads * HEAD), lambda i: (i, 0)),
        out_shape=jax.ShapeDtypeStruct((width, kinds * heads * HEAD), jnp.bfloat16),
        cost_estimate=pl.CostEstimate(flops=20_000_000_000, bytes_accessed=50_000_000, transcendentals=0),
    )(w_qkv)


ANY = pl.BlockSpec(memory_space=pl.ANY)
VMEM = pl.BlockSpec(memory_space=pltpu.VMEM)
SMEM = pl.BlockSpec(memory_space=pltpu.SMEM)


def run_attention(layer, first, heads, idx, sources, gain, shift, bias, wq_own, wq_par, wo_own, wo_par):
    flops = 2 * SEQ * WIDTH * heads * HEAD * 8 + 8 * SEQ * SEQ * heads * HEAD
    return pl.pallas_call(
        functools.partial(attention_stage, layer, first, heads),
        in_specs=[SMEM] + [ANY] * len(sources) + [VMEM] * 3 + [ANY] * 4,
        out_specs=[ANY, ANY],
        out_shape=[jax.ShapeDtypeStruct((SEQ, WIDTH), jnp.bfloat16), jax.ShapeDtypeStruct((SEQ, WIDTH), jnp.float32)],
        scratch_shapes=[
            pltpu.VMEM((SEQ, WIDTH), jnp.float32),
            pltpu.VMEM((SEQ, WIDTH), jnp.bfloat16),
            pltpu.VMEM((SEQ, 2 * heads * HEAD), jnp.bfloat16),
            pltpu.VMEM((2, 3, SEQ, 256), jnp.bfloat16),
            pltpu.VMEM((2, 3, WIDTH, 256), jnp.bfloat16),
            pltpu.VMEM((3, 2, heads * HEAD, TILE), jnp.bfloat16),
            pltpu.VMEM((2, SEQ, TILE), jnp.bfloat16),
            pltpu.SemaphoreType.DMA((2, CHUNKS)),
            pltpu.SemaphoreType.DMA((2,)),
            pltpu.SemaphoreType.DMA((3,)),
            pltpu.SemaphoreType.DMA((2, 2)),
        ],
        compiler_params=pltpu.CompilerParams(vmem_limit_bytes=VMEM_LIMIT),
        cost_estimate=pl.CostEstimate(flops=flops, bytes_accessed=100_000_000, transcendentals=SEQ * SEQ * heads * 2),
    )(idx, *sources, gain, shift, bias, wq_own, wq_par, wo_own, wo_par)


def run_mlp(layer, last, idx, kept, got, gain, shift, bias_up, bias, up_own, up_par, down_own, down_par):
    rows = SEQ // 2 if last else SEQ
    flops = 8 * SEQ * WIDTH * up_own.shape[2]
    return pl.pallas_call(
        functools.partial(mlp_stage, layer, last),
        in_specs=[SMEM] + [ANY] * 2 + [VMEM] * 4 + [ANY] * 4,
        out_specs=[ANY, ANY],
        out_shape=[jax.ShapeDtypeStruct((rows, WIDTH), jnp.bfloat16), jax.ShapeDtypeStruct((rows, WIDTH), jnp.float32)],
        scratch_shapes=[
            pltpu.VMEM((SEQ, WIDTH), jnp.float32),
            pltpu.VMEM((SEQ, WIDTH), jnp.bfloat16),
            pltpu.VMEM((2, SEQ, up_own.shape[2]), jnp.bfloat16),
            pltpu.VMEM((4, WIDTH, TILE), jnp.bfloat16),
            pltpu.VMEM((2, SEQ, TILE), jnp.bfloat16),
            pltpu.SemaphoreType.DMA((2, CHUNKS)),
            pltpu.SemaphoreType.DMA((4,)),
            pltpu.SemaphoreType.DMA((2, 2)),
        ],
        compiler_params=pltpu.CompilerParams(vmem_limit_bytes=VMEM_LIMIT),
        cost_estimate=pl.CostEstimate(flops=flops, bytes_accessed=160_000_000, transcendentals=2 * SEQ * up_own.shape[2]),
    )(idx, kept, got, gain, shift, bias_up, bias, up_own, up_par, down_own, down_par)


ORDER = ([("a", 0, j) for j in range(4)] + [("m", 0, j) for j in range(4)]
         + [("a", 1, j) for j in range(4)] + [("m", 1, j) for j in range(4)])


def solution(mesh):
    across = [(i, i ^ 2) for i in range(4)]
    beside = [(i, i ^ 1) for i in range(4)]

    def swap_core(value):
        return lax.ppermute(value, "tp", beside)

    def body(x_local, ln1_gain, ln1_bias, ln2_gain, ln2_bias, w_qkv, w_out, b_out, w_up, b_up, w_down, b_down):
        batch, rows, width = x_local.shape
        layers = w_qkv.shape[0]
        heads = w_qkv.shape[3]
        mine = batch // 2
        me = lax.axis_index("tp")
        core = lax.rem(me, 2)
        chip = me // 2
        idx = jnp.stack([core, chip]).astype(jnp.int32)

        x_pairs = x_local.reshape(2, mine, rows, width)
        pieces = [x_pairs[:, j] for j in range(mine)]
        *pieces, w_qkv = lax.optimization_barrier((*pieces, w_qkv))
        tokens = [lax.all_gather(piece, "tp", axis=1, tiled=True) for piece in pieces]
        b_up_par = swap_core(b_up)

        out_own = w_out.reshape(layers, heads * HEAD, width)
        qkv_own, qkv_par = [], []
        for l in range(layers):
            qkv_own.append(run_flatten(l, w_qkv))
            qkv_par.append(swap_core(qkv_own[l]))
        out_par = swap_core(out_own)
        up_par = swap_core(w_up)
        down_par = swap_core(w_down)
        up_bias = jnp.stack([b_up, b_up_par], axis=1).reshape(layers, -1, 1, TILE)

        state = [None] * mine
        finals = [None] * mine
        for kind, l, j in ORDER:
            last = l == layers - 1
            if kind == "a":
                sources = (tokens[j],) if l == 0 else state[j]
                send, keep = run_attention(l, l == 0, heads, idx, sources, ln1_gain[l:l + 1], ln1_bias[l:l + 1], b_out[l:l + 1],
                                           qkv_own[l], qkv_par[l], out_own, out_par)
            else:
                send, keep = run_mlp(l, last, idx, *state[j], ln2_gain[l:l + 1], ln2_bias[l:l + 1], up_bias[l], b_down[l:l + 1],
                                     w_up, up_par, w_down, down_par)
            got = lax.ppermute(send, "tp", across)
            state[j] = (keep, got)
            if kind == "m" and last:
                done = (keep + got.astype(jnp.float32)).astype(jnp.bfloat16).reshape(2, rows, width)
                stay = lax.dynamic_index_in_dim(done, core, 0, keepdims=False)
                go = swap_core(lax.dynamic_index_in_dim(done, 1 - core, 0, keepdims=False))
                finals[j] = (stay, go)
        first = jnp.stack([jnp.where(core == 0, s, g) for s, g in finals])
        second = jnp.stack([jnp.where(core == 0, g, s) for s, g in finals])
        return jnp.concatenate([first, second], axis=0)


    rows_spec = P("dp", "tp", None)
    in_specs = (rows_spec, P(), P(), P(), P(), P(None, None, None, "tp", None), P(None, "tp", None, None), P(), P(None, None, "tp"), P(None, "tp"), P(None, "tp", None), P())
    return jax.shard_map(body, mesh=mesh, in_specs=in_specs, out_specs=rows_spec, check_vma=False)
```
